128 devices in a mesh: left: 32 (over z, y_lo, x), right: 4 (over y_hi, core).
Axes of the slice: x: 4, y: 4 (y_hi: 2, y_lo: 2; y = y_hi * 2 + y_lo), z: 4, core: 2. Of those that a mesh axis runs over, the one named last changes fastest.
Arguments:
- density: float32 [512, 512, 2048], P(None, 'left', 'right'), may hold values from -6 to 6
- symbol_x: float32 [512], replicated, may hold values from 0.3 to 3
- symbol_y: float32 [512], replicated, may hold values from 0.3 to 3
- symbol_z: float32 [2048], replicated, may hold values from 0.3 to 3
Outputs:
- spectrum: float32 [512, 512, 2048], P('left', 'right')
The draws below stay inside these ranges and needn't reach their ends.
All inputs are finite; a program needn't handle non-finite values.
Results may differ from the reference program's by a relative error of at most 0.00007.
Values sent between devices are 32-bit elements; how exact they have to be, the bound alone decides.
A program may use at most 192 MiB of HBM per device.

```python
import jax
import jax.numpy as jnp
from jax import lax

GRID_X = 512
GRID_Y = 512
GRID_Z = 2048


def level_of(rng, shape, split, smallest, high):
    def one(dim, parts):
        steps = jax.random.uniform(jax.random.fold_in(jax.random.fold_in(rng, 6), dim), (parts,), jnp.float32, smallest / len(split), high / len(split))
        return jnp.repeat(jnp.exp(steps), shape[dim] // parts).reshape((-1,) + (1,) * (len(shape) - dim - 1))

    level = one(*split[0])
    for cut in split[1:]:
        level = level * one(*cut)
    return level


def centred(key, shape, scale, most, pieces=(), kind=jnp.bfloat16):
    level = level_of(key, shape, pieces, -0.22, 0.18) if pieces else 1.0
    array = jax.random.normal(key, shape, jnp.float32) * scale * level
    return jnp.minimum(jnp.maximum(array, -most), most).astype(kind)


def setup_inputs(seed: int = 0) -> dict:
    streams_of = jax.random.split(jax.random.key(seed), 5)
    density = centred(streams_of[0], (GRID_X, GRID_Y, GRID_Z), 1.0, 6.0, ((1, 32), (2, 4)), jnp.float32)
    symbol_x = jnp.clip(jax.random.uniform(streams_of[1], (GRID_X,), jnp.float32, 0.3, 3.0), 0.3, 3.0)
    symbol_y = jnp.clip(jax.random.uniform(streams_of[2], (GRID_Y,), jnp.float32, 0.3, 3.0), 0.3, 3.0)
    symbol_z = jnp.clip(jax.random.uniform(streams_of[3], (GRID_Z,), jnp.float32, 0.3, 3.0), 0.3, 3.0)
    return {"density": density, "symbol_x": symbol_x, "symbol_y": symbol_y, "symbol_z": symbol_z}


def mode_table(count):
    rank = jnp.arange(count)
    angle = 2.0 * jnp.pi / count * (rank[:, None] * rank[None, :] % count).astype(jnp.float32)
    return (jnp.cos(angle) + jnp.sin(angle)) * count ** (-0.5)

def transform_dim(values, dim):
    moved = jnp.tensordot(values, mode_table(values.shape[dim]), axes=([dim], [0]), precision=lax.Precision.HIGHEST)
    return jnp.moveaxis(moved, -1, dim)

def reference(density, symbol_x, symbol_y, symbol_z):
    spectrum = density
    spectrum = transform_dim(spectrum, 0)
    spectrum = transform_dim(spectrum, 1)
    spectrum = transform_dim(spectrum, 2)
    symbol = symbol_x[:, None, None] + symbol_y[None, :, None] + symbol_z[None, None, :]
    spectrum = spectrum * lax.rsqrt(symbol)
    return spectrum
```

```python
import jax
import jax.numpy as jnp
import numpy as np
from jax import lax
from jax.experimental import pallas as pl
from jax.experimental.pallas import tpu as pltpu
from jax.sharding import PartitionSpec as P

MESH = pl.DeviceIdType.MESH
F32 = jnp.float32
BF16 = jnp.bfloat16
LANES = 128


def halves(value):
    high = value.astype(BF16)
    return high, (value - high.astype(F32)).astype(BF16)


def small_table(count):
    rank = np.arange(count)
    angle = 2.0 * np.pi / count * (rank[:, None] * rank[None, :] % count)
    table = ((np.cos(angle) + np.sin(angle)) * count ** (-0.5)).astype(np.float32)
    high = table.astype(BF16)
    low = (table - high.astype(np.float32)).astype(BF16)
    return np.stack([high, low])


def factor_tables(count, inner):
    rest, col = np.arange(inner), np.arange(count)
    angle = 2.0 * np.pi / count * (rest[:, None] * col[None, :] % count)
    scale = count ** (-0.5)
    plus = (np.cos(angle) + np.sin(angle)) * scale
    minus = (np.cos(angle) - np.sin(angle)) * scale
    outer = np.arange(count // inner)
    angle = 2.0 * np.pi / count * (outer[:, None] * inner * np.arange(LANES)[None, :] % count)
    return np.stack([plus, minus]).astype(np.float32), np.stack([np.cos(angle), np.sin(angle)]).astype(np.float32)


def dot(a, b):
    return jnp.dot(a, b, preferred_element_type=F32)


def make_kernel(n_left, n_right, size_x, size_y, size_z):
    part_x, part_y, rows_y, part_z = size_x // n_left, size_y // n_left, size_y // n_right, size_z // n_right
    inner = 64

    def partner(me, step):
        x = step & 3
        k = step >> 2
        z = (k ^ x) & 3
        y = ((k >> 2) ^ (x >> 1)) & 1
        return me ^ ((z << 3) | (y << 2) | x)

    def kernel(
        field, small, cas, turn,
        lines_y, lines_z, result,
        held, big_high, big_low, taken, stacked, given,
        load_sem, send_x, recv_x, keep_x, send_y, recv_y, keep_y, z_in_sem, z_out_sem,
    ):
        left = lax.axis_index("left")
        right = lax.axis_index("right")

        def load_x(y, slot):
            return pltpu.make_async_copy(field.at[:, y, :], taken.at[slot], load_sem.at[slot])

        load_x(0, 0).start()

        barrier = pltpu.get_barrier_semaphore()

        @pl.loop(1, n_left)
        def _(step):
            pl.semaphore_signal(barrier, inc=1, device_id={"left": partner(left, step)}, device_id_type=MESH)

        @pl.loop(1, n_right)
        def _(step):
            pl.semaphore_signal(barrier, inc=1, device_id={"right": right ^ step}, device_id_type=MESH)

        pl.semaphore_wait(barrier, n_left + n_right - 2)

        def transform(slot, out):
            for n in range(0, part_z, 256):
                high, low = halves(taken[slot, :, n : n + 256])
                held[out, :, n : n + 256] = dot(small[0], high) + dot(small[0], low) + dot(small[1], high)

        @pl.loop(0, part_y)
        def _(y):
            slot = y & 1

            @pl.when(y + 1 < part_y)
            def _():
                load_x(y + 1, 1 - slot).start()

            load_x(y, slot).wait()
            transform(slot, y)
            to = left * part_y + y

            @pl.loop(1, n_left)
            def _(step):
                peer = partner(left, step)
                pltpu.make_async_remote_copy(
                    src_ref=held.at[y, pl.ds(peer * part_x, part_x)],
                    dst_ref=lines_y.at[to],
                    send_sem=send_x,
                    recv_sem=recv_x,
                    device_id={"left": peer},
                    device_id_type=MESH,
                ).start()

            pltpu.make_async_copy(held.at[y, pl.ds(left * part_x, part_x)], lines_y.at[to], keep_x).start()

        @pl.loop(0, size_z // inner)
        def _(outer):
            cos = turn[0, pl.ds(outer, 1), :]
            sin = turn[1, pl.ds(outer, 1), :]
            for c in range(0, size_z, LANES):
                value = cas[0, :, c : c + LANES] * cos + cas[1, :, c : c + LANES] * sin
                high, low = halves(value)
                big_high[pl.ds(outer * inner, inner), c : c + LANES] = high
                big_low[pl.ds(outer * inner, inner), c : c + LANES] = low

        own = lines_y.at[pl.ds(0, part_y)]
        pltpu.make_async_copy(own, own, keep_x).wait()
        others = lines_y.at[pl.ds(0, size_y - part_y)]
        pltpu.make_async_copy(others, others, send_x).wait()
        pltpu.make_async_copy(others, others, recv_x).wait()

        def load_y(k, slot):
            return pltpu.make_async_copy(lines_y.at[:, k, :], taken.at[slot], load_sem.at[slot])

        load_y(0, 0).start()

        @pl.loop(0, part_x)
        def _(k):
            slot = k & 1

            @pl.when(k + 1 < part_x)
            def _():
                load_y(k + 1, 1 - slot).start()

            load_y(k, slot).wait()
            transform(slot, k)
            columns = pl.ds(pl.multiple_of(right * part_z, part_z), part_z)

            @pl.loop(0, n_right - 1)
            def _(step):
                peer = right ^ lax.rem(step + 1, n_right - 1) + 1
                pltpu.make_async_remote_copy(
                    src_ref=held.at[k, pl.ds(peer * rows_y, rows_y)],
                    dst_ref=lines_z.at[k, :, columns],
                    send_sem=send_y,
                    recv_sem=recv_y.at[k],
                    device_id={"right": peer},
                    device_id_type=MESH,
                ).start()

            pltpu.make_async_copy(held.at[k, pl.ds(right * rows_y, rows_y)], lines_z.at[k, :, columns], keep_y.at[k]).start()

        def store_z(k, slot):
            return pltpu.make_async_copy(given.at[slot], result.at[k], z_out_sem.at[slot])

        @pl.loop(0, part_x)
        def _(k):
            slot = k & 1
            mine = lines_z.at[k, :, pl.ds(0, part_z)]
            pltpu.make_async_copy(mine, mine, keep_y.at[k]).wait()
            theirs = lines_z.at[k, :, pl.ds(0, size_z - part_z)]
            pltpu.make_async_copy(theirs, theirs, recv_y.at[k]).wait()
            for r in range(n_right):
                pltpu.make_async_copy(
                    lines_z.at[k, :, pl.ds(r * part_z, part_z)], taken.at[0, pl.ds(r * rows_y, rows_y)], z_in_sem.at[r]
                ).start()
            for r in range(n_right):
                pltpu.make_async_copy(
                    lines_z.at[k, :, pl.ds(r * part_z, part_z)], taken.at[0, pl.ds(r * rows_y, rows_y)], z_in_sem.at[r]
                ).wait()
                high, low = halves(taken[0, r * rows_y : (r + 1) * rows_y, :])
                stacked[:rows_y, r * part_z : (r + 1) * part_z] = high
                stacked[rows_y:, r * part_z : (r + 1) * part_z] = low

            @pl.when(k >= 2)
            def _():
                store_z(k - 2, slot).wait()

            @pl.loop(0, size_z, step=256)
            def _(n):
                cut = pl.ds(pl.multiple_of(n, 256), 256)
                both = dot(stacked[...], big_high[:, cut])
                given[slot, :, cut] = both[:rows_y] + both[rows_y:] + dot(stacked[:rows_y, :], big_low[:, cut])

            store_z(k, slot).start()

        for k in (part_x - 2, part_x - 1):
            store_z(k, k & 1).wait()
        sent = result.at[pl.ds(0, part_x), :, pl.ds(0, size_z - part_z)]
        pltpu.make_async_copy(sent, sent, send_y).wait()

    held_rows = max(part_x, part_y)
    anywhere = pl.BlockSpec(memory_space=pl.ANY)
    inside = pl.BlockSpec(memory_space=pltpu.VMEM)
    dma = pltpu.SemaphoreType.DMA
    return pl.pallas_call(
        kernel,
        out_shape=[
            jax.ShapeDtypeStruct((size_y, part_x, part_z), F32),
            jax.ShapeDtypeStruct((part_x, rows_y, size_z), F32),
            jax.ShapeDtypeStruct((part_x, rows_y, size_z), F32),
        ],
        in_specs=[anywhere, inside, inside, inside],
        out_specs=[anywhere] * 3,
        scratch_shapes=[
            pltpu.VMEM((held_rows, size_x, part_z), F32),
            pltpu.VMEM((size_z, size_z), BF16),
            pltpu.VMEM((size_z, size_z), BF16),
            pltpu.VMEM((2, size_x, part_z), F32),
            pltpu.VMEM((2 * rows_y, size_z), BF16),
            pltpu.VMEM((2, rows_y, size_z), F32),
            dma((2,)),
            dma, dma, dma,
            dma, dma((part_x,)), dma((part_x,)),
            dma((n_right,)), dma((2,)),
        ],
        compiler_params=pltpu.CompilerParams(
            collective_id=0, has_side_effects=True, vmem_limit_bytes=62 * 1024 * 1024
        ),
        name="hartley",
    )


def solution(mesh):
    n_left, n_right = mesh.shape["left"], mesh.shape["right"]

    def per_device(density, symbol_x, symbol_y, symbol_z):
        size_x, size_y, size_z = density.shape[0], density.shape[1] * n_left, density.shape[2] * n_right
        small = jnp.asarray(small_table(size_x))
        cas, turn = (jnp.asarray(t) for t in factor_tables(size_z, 64))
        result = make_kernel(n_left, n_right, size_x, size_y, size_z)(density, small, cas, turn)[2]
        share_x, share_y = size_x // n_left, size_y // n_right
        part_x = lax.dynamic_slice_in_dim(symbol_x, lax.axis_index("left") * share_x, share_x)
        part_y = lax.dynamic_slice_in_dim(symbol_y, lax.axis_index("right") * share_y, share_y)
        symbol = part_x[:, None, None] + part_y[None, :, None] + symbol_z[None, None, :]
        return result * lax.rsqrt(symbol)

    return jax.shard_map(
        per_device,
        mesh=mesh,
        in_specs=(P(None, "left", "right"), P(), P(), P()),
        out_specs=P("left", "right", None),
        check_vma=False,
    )
```

```python
import jax
import jax.numpy as jnp
import numpy as np
from jax import lax
from jax.experimental import pallas as pl
from jax.experimental.pallas import tpu as pltpu
from jax.sharding import PartitionSpec as P

MESH = pl.DeviceIdType.MESH
F32 = jnp.float32
BF16 = jnp.bfloat16
LANES = 128


def halves(value):
    high = value.astype(BF16)
    return high, (value - high.astype(F32)).astype(BF16)


def small_table(count):
    rank = np.arange(count)
    angle = 2.0 * np.pi / count * (rank[:, None] * rank[None, :] % count)
    table = ((np.cos(angle) + np.sin(angle)) * count ** (-0.5)).astype(np.float32)
    high = table.astype(BF16)
    low = (table - high.astype(np.float32)).astype(BF16)
    return np.stack([high, low])


def factor_tables(count, inner):
    rest, col = np.arange(inner), np.arange(count)
    angle = 2.0 * np.pi / count * (rest[:, None] * col[None, :] % count)
    scale = count ** (-0.5)
    plus = (np.cos(angle) + np.sin(angle)) * scale
    minus = (np.cos(angle) - np.sin(angle)) * scale
    outer = np.arange(count // inner)
    angle = 2.0 * np.pi / count * (outer[:, None] * inner * np.arange(LANES)[None, :] % count)
    return np.stack([plus, minus]).astype(np.float32), np.stack([np.cos(angle), np.sin(angle)]).astype(np.float32)


def dot(a, b):
    return jnp.dot(a, b, preferred_element_type=F32)


def make_kernel(n_left, n_right, size_x, size_y, size_z):
    part_x, part_y, rows_y, part_z = size_x // n_left, size_y // n_left, size_y // n_right, size_z // n_right
    half_x, half_z = part_x // 2, size_z // 2
    inner = 64

    def partner(me, step):
        x = step & 3
        k = step >> 2
        z = (k ^ x) & 3
        y = ((k >> 2) ^ (x >> 1)) & 1
        return me ^ ((z << 3) | (y << 2) | x)

    def kernel(
        field, small_far, cas_far, turn_far, sym_x, sym_y, sym_z,
        lines_y, lines_z, result,
        held, big_high, big_low, taken, line_in, stacked, partial, small, cas, turn, column,
        load_sem, table_sem, send_x, recv_x, keep_x, send_y, near_y, far_y, keep_y, line_sem,
    ):
        left = lax.axis_index("left")
        right = lax.axis_index("right")

        def load_x(y, slot):
            return pltpu.make_async_copy(field.at[:, y, :], taken.at[slot], load_sem.at[slot])

        tables = [
            pltpu.make_async_copy(far, near, table_sem.at[i])
            for i, (far, near) in enumerate(((small_far, small), (cas_far, cas), (turn_far, turn)))
        ]
        load_x(0, 0).start()
        for copy in tables:
            copy.start()

        barrier = pltpu.get_barrier_semaphore()

        @pl.loop(1, n_left)
        def _(step):
            pl.semaphore_signal(barrier, inc=1, device_id={"left": partner(left, step)}, device_id_type=MESH)

        @pl.loop(1, n_right)
        def _(step):
            pl.semaphore_signal(barrier, inc=1, device_id={"right": right ^ step}, device_id_type=MESH)

        tables[0].wait()
        pl.semaphore_wait(barrier, n_left + n_right - 2)

        def product(slot, n):
            high, low = halves(taken[slot, :, n : n + 256])
            return dot(small[0], high) + dot(small[0], low) + dot(small[1], high)

        def send_half(y, h):
            to = left * part_y + y

            @pl.loop(1, n_left)
            def _(step):
                peer = partner(left, step)
                pltpu.make_async_remote_copy(
                    src_ref=held.at[y, pl.ds(peer * part_x + h * half_x, half_x)],
                    dst_ref=lines_y.at[to, pl.ds(h * half_x, half_x)],
                    send_sem=send_x,
                    recv_sem=recv_x.at[h],
                    device_id={"left": peer},
                    device_id_type=MESH,
                ).start()

            pltpu.make_async_copy(
                held.at[y, pl.ds(left * part_x + h * half_x, half_x)],
                lines_y.at[to, pl.ds(h * half_x, half_x)],
                keep_x.at[h],
            ).start()

        @pl.loop(0, part_y)
        def _(y):
            slot = y & 1

            @pl.when(y + 1 < part_y)
            def _():
                load_x(y + 1, 1 - slot).start()

            load_x(y, slot).wait()
            for n in range(0, part_z, 256):
                held[y, :, n : n + 256] = product(slot, n)
            send_half(y, 0)

        @pl.loop(0, part_y)
        def _(y):
            send_half(y, 1)

        tables[1].wait()
        tables[2].wait()

        @pl.loop(0, size_z // inner)
        def _(outer):
            cos = turn[0, pl.ds(outer, 1), :]
            sin = turn[1, pl.ds(outer, 1), :]
            for c in range(0, size_z, LANES):
                value = cas[0, :, c : c + LANES] * cos + cas[1, :, c : c + LANES] * sin
                high, low = halves(value)
                big_high[pl.ds(outer * inner, inner), c : c + LANES] = high
                big_low[pl.ds(outer * inner, inner), c : c + LANES] = low

        rows = pl.multiple_of(right * rows_y, rows_y)
        column[...] = jnp.broadcast_to(sym_y[:, pl.ds(rows, rows_y)], (rows_y, rows_y)).T

        def arrived_x(h):
            part = pl.ds(h * half_x, half_x)
            own = lines_y.at[pl.ds(0, part_y), part]
            pltpu.make_async_copy(own, own, keep_x.at[h]).wait()
            others = lines_y.at[pl.ds(0, size_y - part_y), part]
            pltpu.make_async_copy(others, others, recv_x.at[h]).wait()

        def load_y(k, slot):
            return pltpu.make_async_copy(lines_y.at[:, k, :], taken.at[slot], load_sem.at[slot])

        columns = pl.ds(pl.multiple_of(right * part_z, part_z), part_z)

        def send_plane(k):
            for flip, sem in ((2, far_y), (3, far_y), (1, near_y)):
                peer = right ^ flip
                pltpu.make_async_remote_copy(
                    src_ref=result.at[k, :, pl.ds(pl.multiple_of(peer * part_z, part_z), part_z)],
                    dst_ref=lines_z.at[k, :, columns],
                    send_sem=send_y.at[k],
                    recv_sem=sem.at[k],
                    device_id={"right": peer},
                    device_id_type=MESH,
                ).start()
            pltpu.make_async_copy(result.at[k, :, columns], lines_z.at[k, :, columns], keep_y.at[k]).start()

        def transform_y(first, last, send):
            load_y(first, first & 1).start()

            @pl.loop(first, last)
            def _(k):
                slot = k & 1

                @pl.when(k + 1 < last)
                def _():
                    load_y(k + 1, 1 - slot).start()

                load_y(k, slot).wait()
                for n in range(0, part_z, 256):
                    value = product(slot, n)
                    for r in range(n_right):
                        result[k, :, r * part_z + n : r * part_z + n + 256] = value[r * rows_y : (r + 1) * rows_y]
                if send:
                    send_plane(k)

        arrived_x(0)
        transform_y(0, half_x, False)
        arrived_x(1)

        @pl.loop(0, half_x)
        def _(k):
            send_plane(k)

        transform_y(half_x, part_x, True)

        here = pl.multiple_of((right >> 1) * half_z, half_z)
        there = pl.multiple_of(half_z - here, half_z)

        def line(k, side, start):
            return pltpu.make_async_copy(lines_z.at[k, :, pl.ds(start, half_z)], line_in.at[side], line_sem.at[side])

        def stack(side):
            high, low = halves(line_in[side])
            stacked[side, :rows_y] = high
            stacked[side, rows_y:] = low

        def product_z(side, start, cut):
            both = dot(stacked[side], big_high[pl.ds(start, half_z), cut])
            return both[:rows_y] + both[rows_y:] + dot(stacked[side, :rows_y], big_low[pl.ds(start, half_z), cut])

        @pl.loop(0, part_x)
        def _(k):
            mine = lines_z.at[k, :, pl.ds(0, part_z)]
            pltpu.make_async_copy(mine, mine, keep_y.at[k]).wait()
            pltpu.make_async_copy(mine, mine, near_y.at[k]).wait()
            line(k, 0, here).start()
            line(k, 0, here).wait()
            stack(0)

            @pl.loop(0, size_z, step=512)
            def _(n):
                cut = pl.ds(pl.multiple_of(n, 512), 512)
                partial[:, cut] = product_z(0, here, cut)

            theirs = lines_z.at[k, :, pl.ds(0, half_z)]
            pltpu.make_async_copy(theirs, theirs, far_y.at[k]).wait()
            line(k, 1, there).start()
            sent = lines_z.at[k, :, pl.ds(0, size_z - part_z)]
            pltpu.make_async_copy(sent, sent, send_y.at[k]).wait()
            line(k, 1, there).wait()
            stack(1)
            sym_xy = sym_x[left * part_x + k] + column[...]

            @pl.loop(0, size_z, step=512)
            def _(n):
                cut = pl.ds(pl.multiple_of(n, 512), 512)
                total = partial[:, cut] + product_z(1, there, cut)
                for c in range(0, 512, LANES):
                    some = pl.ds(pl.multiple_of(n + c, LANES), LANES)
                    result[k, :, some] = total[:, c : c + LANES] * lax.rsqrt(sym_xy + sym_z[:, some])

        others = lines_y.at[pl.ds(0, size_y - part_y)]
        pltpu.make_async_copy(others, others, send_x).wait()

    far = pl.BlockSpec(memory_space=pltpu.HBM)
    inside = pl.BlockSpec(memory_space=pltpu.VMEM)
    dma = pltpu.SemaphoreType.DMA
    return pl.pallas_call(
        kernel,
        out_shape=[
            jax.ShapeDtypeStruct((size_y, part_x, part_z), F32),
            jax.ShapeDtypeStruct((part_x, rows_y, size_z), F32),
            pltpu.VMEM((part_x, rows_y, size_z), F32),
        ],
        in_specs=[far] * 4 + [pl.BlockSpec(memory_space=pltpu.SMEM), inside, inside],
        out_specs=[far, far, inside],
        scratch_shapes=[
            pltpu.VMEM((part_y, size_x, part_z), F32),
            pltpu.VMEM((size_z, size_z), BF16),
            pltpu.VMEM((size_z, size_z), BF16),
            pltpu.VMEM((2, size_x, part_z), F32),
            pltpu.VMEM((2, rows_y, half_z), F32),
            pltpu.VMEM((2, 2 * rows_y, half_z), BF16),
            pltpu.VMEM((rows_y, size_z), F32),
            pltpu.VMEM((2, size_x, size_x), BF16),
            pltpu.VMEM((2, inner, size_z), F32),
            pltpu.VMEM((2, size_z // inner, LANES), F32),
            pltpu.VMEM((rows_y, rows_y), F32),
            dma((2,)), dma((3,)),
            dma, dma((2,)), dma((2,)),
            dma((part_x,)), dma((part_x,)), dma((part_x,)), dma((part_x,)),
            dma((2,)),
        ],
        compiler_params=pltpu.CompilerParams(
            collective_id=0, has_side_effects=True, vmem_limit_bytes=46 * 1024 * 1024
        ),
        name="hartley",
    )


def solution(mesh):
    n_left, n_right = mesh.shape["left"], mesh.shape["right"]

    def per_device(density, symbol_x, symbol_y, symbol_z):
        size_x, size_y, size_z = density.shape[0], density.shape[1] * n_left, density.shape[2] * n_right
        small = jnp.asarray(small_table(size_x))
        cas, turn = (jnp.asarray(t) for t in factor_tables(size_z, 64))
        kernel = make_kernel(n_left, n_right, size_x, size_y, size_z)
        return kernel(density, small, cas, turn, symbol_x, symbol_y[None, :], symbol_z[None, :])[2]

    return jax.shard_map(
        per_device,
        mesh=mesh,
        in_specs=(P(None, "left", "right"), P(), P(), P()),
        out_specs=P("left", "right", None),
        check_vma=False,
    )
```

```python
import jax
import jax.numpy as jnp
import numpy as np
from jax import lax
from jax.experimental import pallas as pl
from jax.experimental.pallas import tpu as pltpu
from jax.sharding import PartitionSpec as P

MESH = pl.DeviceIdType.MESH
F32 = jnp.float32
BF16 = jnp.bfloat16
LANES = 128


def halves(value):
    high = value.astype(BF16)
    return high, (value - high.astype(F32)).astype(BF16)


def small_table(count):
    rank = np.arange(count)
    angle = 2.0 * np.pi / count * (rank[:, None] * rank[None, :] % count)
    table = ((np.cos(angle) + np.sin(angle)) * count ** (-0.5)).astype(np.float32)
    high = table.astype(BF16)
    low = (table - high.astype(np.float32)).astype(BF16)
    return np.stack([high, low])


def factor_tables(count, inner):
    rest, col = np.arange(inner), np.arange(count)
    angle = 2.0 * np.pi / count * (rest[:, None] * col[None, :] % count)
    scale = count ** (-0.5)
    plus = (np.cos(angle) + np.sin(angle)) * scale
    minus = (np.cos(angle) - np.sin(angle)) * scale
    outer = np.arange(count // inner)
    angle = 2.0 * np.pi / count * (outer[:, None] * inner * np.arange(LANES)[None, :] % count)
    return np.stack([plus, minus]).astype(np.float32), np.stack([np.cos(angle), np.sin(angle)]).astype(np.float32)


def dot(a, b):
    return jnp.dot(a, b, preferred_element_type=F32)


def make_kernel(n_left, n_right, size_x, size_y, size_z):
    part_x, part_y, rows_y, part_z = size_x // n_left, size_y // n_left, size_y // n_right, size_z // n_right
    half_x, half_z = part_x // 2, size_z // 2
    last_y = max(1, part_y // 4)
    inner = 64

    def partner(me, step):
        x = step & 3
        k = step >> 2
        z = (k ^ x) & 3
        y = ((k >> 2) ^ (x >> 1)) & 1
        return me ^ ((z << 3) | (y << 2) | x)

    def kernel(
        field, small_far, cas_far, turn_far, sym_x, sym_y, sym_z,
        lines_y, lines_z, result,
        held, big_high, big_low, taken, line_in, stacked, partial, small, cas, turn, column,
        load_sem, table_sem, send_x, recv_x, keep_x, send_y, near_y, far_y, keep_y, line_sem,
    ):
        left = lax.axis_index("left")
        right = lax.axis_index("right")

        def load_x(y, slot):
            return pltpu.make_async_copy(field.at[:, y, :], taken.at[slot], load_sem.at[slot])

        tables = [
            pltpu.make_async_copy(far, near, table_sem.at[i])
            for i, (far, near) in enumerate(((small_far, small), (cas_far, cas), (turn_far, turn)))
        ]
        load_x(0, 0).start()
        for copy in tables:
            copy.start()

        barrier = pltpu.get_barrier_semaphore()

        @pl.loop(1, n_left)
        def _(step):
            pl.semaphore_signal(barrier, inc=1, device_id={"left": partner(left, step)}, device_id_type=MESH)

        @pl.loop(1, n_right)
        def _(step):
            pl.semaphore_signal(barrier, inc=1, device_id={"right": right ^ step}, device_id_type=MESH)

        tables[0].wait()
        pl.semaphore_wait(barrier, n_left + n_right - 2)

        def product(slot, n):
            high, low = halves(taken[slot, :, n : n + 256])
            return dot(small[0], high) + dot(small[0], low) + dot(small[1], high)

        def send_half(y, h, sem):
            to = left * part_y + y

            @pl.loop(1, n_left)
            def _(step):
                peer = partner(left, step)
                pltpu.make_async_remote_copy(
                    src_ref=held.at[y, pl.ds(peer * part_x + h * half_x, half_x)],
                    dst_ref=lines_y.at[to, pl.ds(h * half_x, half_x)],
                    send_sem=send_x.at[sem],
                    recv_sem=recv_x.at[h],
                    device_id={"left": peer},
                    device_id_type=MESH,
                ).start()

            pltpu.make_async_copy(
                held.at[y, pl.ds(left * part_x + h * half_x, half_x)],
                lines_y.at[to, pl.ds(h * half_x, half_x)],
                keep_x.at[h],
            ).start()

        @pl.loop(0, part_y)
        def _(y):
            slot = y & 1

            @pl.when(y + 1 < part_y)
            def _():
                load_x(y + 1, 1 - slot).start()

            load_x(y, slot).wait()
            for n in range(0, part_z, 256):
                held[y, :, n : n + 256] = product(slot, n)
            send_half(y, 0, 0)

        @pl.loop(0, part_y - last_y)
        def _(y):
            send_half(y, 1, 1)

        @pl.loop(part_y - last_y, part_y)
        def _(y):
            send_half(y, 1, 2)

        def left_x(sem, planes):
            gone = lines_y.at[pl.ds(0, planes * (n_left - 1)), pl.ds(0, half_x)]
            pltpu.make_async_copy(gone, gone, send_x.at[sem]).wait()

        tables[1].wait()
        tables[2].wait()

        @pl.loop(0, size_z // inner)
        def _(outer):
            cos = turn[0, pl.ds(outer, 1), :]
            sin = turn[1, pl.ds(outer, 1), :]
            for c in range(0, size_z, LANES):
                value = cas[0, :, c : c + LANES] * cos + cas[1, :, c : c + LANES] * sin
                high, low = halves(value)
                big_high[pl.ds(outer * inner, inner), c : c + LANES] = high
                big_low[pl.ds(outer * inner, inner), c : c + LANES] = low

        rows = pl.multiple_of(right * rows_y, rows_y)
        column[...] = jnp.broadcast_to(sym_y[:, pl.ds(rows, rows_y)], (rows_y, rows_y)).T

        def arrived_x(h):
            part = pl.ds(h * half_x, half_x)
            own = lines_y.at[pl.ds(0, part_y), part]
            pltpu.make_async_copy(own, own, keep_x.at[h]).wait()
            others = lines_y.at[pl.ds(0, size_y - part_y), part]
            pltpu.make_async_copy(others, others, recv_x.at[h]).wait()

        def load_y(k, slot):
            return pltpu.make_async_copy(lines_y.at[:, k, :], taken.at[slot], load_sem.at[slot])

        columns = pl.ds(pl.multiple_of(right * part_z, part_z), part_z)

        def send_plane(k):
            for flip, sem in ((2, far_y), (3, far_y), (1, near_y)):
                peer = right ^ flip
                pltpu.make_async_remote_copy(
                    src_ref=result.at[k, :, pl.ds(pl.multiple_of(peer * part_z, part_z), part_z)],
                    dst_ref=lines_z.at[k, :, columns],
                    send_sem=send_y.at[k],
                    recv_sem=sem.at[k],
                    device_id={"right": peer},
                    device_id_type=MESH,
                ).start()
            pltpu.make_async_copy(result.at[k, :, columns], lines_z.at[k, :, columns], keep_y.at[k]).start()

        def transform_y(first, last, send):
            load_y(first, first & 1).start()

            @pl.loop(first, last)
            def _(k):
                slot = k & 1

                @pl.when(k + 1 < last)
                def _():
                    load_y(k + 1, 1 - slot).start()

                load_y(k, slot).wait()
                for n in range(0, part_z, 256):
                    value = product(slot, n)
                    for r in range(n_right):
                        result[k, :, r * part_z + n : r * part_z + n + 256] = value[r * rows_y : (r + 1) * rows_y]
                if send:
                    send_plane(k)

        arrived_x(0)
        transform_y(0, half_x, False)

        left_x(0, part_y)
        left_x(1, part_y - last_y)

        @pl.loop(0, half_x)
        def _(k):
            send_plane(k)

        arrived_x(1)
        transform_y(half_x, part_x, True)

        here = pl.multiple_of((right >> 1) * half_z, half_z)
        there = pl.multiple_of(half_z - here, half_z)

        def line(k, side, start):
            return pltpu.make_async_copy(lines_z.at[k, :, pl.ds(start, half_z)], line_in.at[side], line_sem.at[side])

        def stack(side):
            high, low = halves(line_in[side])
            stacked[side, :rows_y] = high
            stacked[side, rows_y:] = low

        def product_z(side, start, cut):
            both = dot(stacked[side], big_high[pl.ds(start, half_z), cut])
            return both[:rows_y] + both[rows_y:] + dot(stacked[side, :rows_y], big_low[pl.ds(start, half_z), cut])

        @pl.loop(0, part_x)
        def _(k):
            mine = lines_z.at[k, :, pl.ds(0, part_z)]
            pltpu.make_async_copy(mine, mine, keep_y.at[k]).wait()
            pltpu.make_async_copy(mine, mine, near_y.at[k]).wait()
            line(k, 0, here).start()
            line(k, 0, here).wait()
            stack(0)

            @pl.loop(0, size_z, step=512)
            def _(n):
                cut = pl.ds(pl.multiple_of(n, 512), 512)
                partial[:, cut] = product_z(0, here, cut)

            theirs = lines_z.at[k, :, pl.ds(0, half_z)]
            pltpu.make_async_copy(theirs, theirs, far_y.at[k]).wait()
            line(k, 1, there).start()
            sent = lines_z.at[k, :, pl.ds(0, size_z - part_z)]
            pltpu.make_async_copy(sent, sent, send_y.at[k]).wait()
            line(k, 1, there).wait()
            stack(1)
            sym_xy = sym_x[left * part_x + k] + column[...]

            @pl.loop(0, size_z, step=512)
            def _(n):
                cut = pl.ds(pl.multiple_of(n, 512), 512)
                total = partial[:, cut] + product_z(1, there, cut)
                for c in range(0, 512, LANES):
                    some = pl.ds(pl.multiple_of(n + c, LANES), LANES)
                    result[k, :, some] = total[:, c : c + LANES] * lax.rsqrt(sym_xy + sym_z[:, some])

        left_x(2, last_y)

    far = pl.BlockSpec(memory_space=pltpu.HBM)
    inside = pl.BlockSpec(memory_space=pltpu.VMEM)
    dma = pltpu.SemaphoreType.DMA
    return pl.pallas_call(
        kernel,
        out_shape=[
            jax.ShapeDtypeStruct((size_y, part_x, part_z), F32),
            jax.ShapeDtypeStruct((part_x, rows_y, size_z), F32),
            pltpu.VMEM((part_x, rows_y, size_z), F32),
        ],
        in_specs=[far] * 4 + [pl.BlockSpec(memory_space=pltpu.SMEM), inside, inside],
        out_specs=[far, far, inside],
        scratch_shapes=[
            pltpu.VMEM((part_y, size_x, part_z), F32),
            pltpu.VMEM((size_z, size_z), BF16),
            pltpu.VMEM((size_z, size_z), BF16),
            pltpu.VMEM((2, size_x, part_z), F32),
            pltpu.VMEM((2, rows_y, half_z), F32),
            pltpu.VMEM((2, 2 * rows_y, half_z), BF16),
            pltpu.VMEM((rows_y, size_z), F32),
            pltpu.VMEM((2, size_x, size_x), BF16),
            pltpu.VMEM((2, inner, size_z), F32),
            pltpu.VMEM((2, size_z // inner, LANES), F32),
            pltpu.VMEM((rows_y, rows_y), F32),
            dma((2,)), dma((3,)),
            dma((3,)), dma((2,)), dma((2,)),
            dma((part_x,)), dma((part_x,)), dma((part_x,)), dma((part_x,)),
            dma((2,)),
        ],
        compiler_params=pltpu.CompilerParams(
            collective_id=0, has_side_effects=True, vmem_limit_bytes=46 * 1024 * 1024
        ),
        name="hartley",
    )


def solution(mesh):
    n_left, n_right = mesh.shape["left"], mesh.shape["right"]

    def per_device(density, symbol_x, symbol_y, symbol_z):
        size_x, size_y, size_z = density.shape[0], density.shape[1] * n_left, density.shape[2] * n_right
        small = jnp.asarray(small_table(size_x))
        cas, turn = (jnp.asarray(t) for t in factor_tables(size_z, 64))
        kernel = make_kernel(n_left, n_right, size_x, size_y, size_z)
        return kernel(density, small, cas, turn, symbol_x, symbol_y[None, :], symbol_z[None, :])[2]

    return jax.shard_map(
        per_device,
        mesh=mesh,
        in_specs=(P(None, "left", "right"), P(), P(), P()),
        out_specs=P("left", "right", None),
        check_vma=False,
    )
```

```python
import jax
import jax.numpy as jnp
import numpy as np
from jax import lax
from jax.experimental import pallas as pl
from jax.experimental.pallas import tpu as pltpu
from jax.sharding import PartitionSpec as P

MESH = pl.DeviceIdType.MESH
F32 = jnp.float32
BF16 = jnp.bfloat16
LANES = 128


def halves(value):
    high = value.astype(BF16)
    return high, (value - high.astype(F32)).astype(BF16)


def small_table(count):
    rank = np.arange(count)
    angle = 2.0 * np.pi / count * (rank[:, None] * rank[None, :] % count)
    table = ((np.cos(angle) + np.sin(angle)) * count ** (-0.5)).astype(np.float32)
    high = table.astype(BF16)
    low = (table - high.astype(np.float32)).astype(BF16)
    return np.stack([high, low])


def factor_tables(count, inner):
    rest, col = np.arange(inner), np.arange(count)
    angle = 2.0 * np.pi / count * (rest[:, None] * col[None, :] % count)
    scale = count ** (-0.5)
    plus = (np.cos(angle) + np.sin(angle)) * scale
    minus = (np.cos(angle) - np.sin(angle)) * scale
    outer = np.arange(count // inner)
    angle = 2.0 * np.pi / count * (outer[:, None] * inner * np.arange(LANES)[None, :] % count)
    return np.stack([plus, minus]).astype(np.float32), np.stack([np.cos(angle), np.sin(angle)]).astype(np.float32)


def dot(a, b):
    return jnp.dot(a, b, preferred_element_type=F32)


def make_kernel(n_left, n_right, size_x, size_y, size_z):
    part_x, part_y, rows_y, part_z = size_x // n_left, size_y // n_left, size_y // n_right, size_z // n_right
    half_x, half_z = part_x // 2, size_z // 2
    last_y = max(1, part_y // 4)
    inner = 64

    def partner(me, step):
        x = step & 3
        k = step >> 2
        z = (k ^ x) & 3
        y = ((k >> 2) ^ (x >> 1)) & 1
        return me ^ ((z << 3) | (y << 2) | x)

    def kernel(
        field, small_far, cas_far, turn_far, sym_x, sym_y, sym_z,
        lines_y, lines_z, result,
        held, big_high, big_low, taken, line_in, stacked, partial, small, cas, turn, column,
        load_sem, table_sem, send_x, recv_x, keep_x, send_y, near_y, far_y, keep_y, line_sem,
    ):
        left = lax.axis_index("left")
        right = lax.axis_index("right")

        def load_x(y, slot):
            return pltpu.make_async_copy(field.at[:, y, :], taken.at[slot], load_sem.at[slot])

        tables = [
            pltpu.make_async_copy(far, near, table_sem.at[i])
            for i, (far, near) in enumerate(((small_far, small), (cas_far, cas), (turn_far, turn)))
        ]
        load_x(0, 0).start()
        for copy in tables:
            copy.start()

        barrier = pltpu.get_barrier_semaphore()

        @pl.loop(1, n_left)
        def _(step):
            pl.semaphore_signal(barrier, inc=1, device_id={"left": partner(left, step)}, device_id_type=MESH)

        @pl.loop(1, n_right)
        def _(step):
            pl.semaphore_signal(barrier, inc=1, device_id={"right": right ^ step}, device_id_type=MESH)

        def product(slot, n):
            high, low = halves(taken[slot, :, n : n + 256])
            return dot(small[0], high) + dot(small[0], low) + dot(small[1], high)

        def send_half(y, h, sem):
            to = left * part_y + y

            @pl.loop(1, n_left)
            def _(step):
                peer = partner(left, step)
                pltpu.make_async_remote_copy(
                    src_ref=held.at[y, pl.ds(peer * part_x + h * half_x, half_x)],
                    dst_ref=lines_y.at[to, pl.ds(h * half_x, half_x)],
                    send_sem=send_x.at[sem],
                    recv_sem=recv_x.at[h],
                    device_id={"left": peer},
                    device_id_type=MESH,
                ).start()

            pltpu.make_async_copy(
                held.at[y, pl.ds(left * part_x + h * half_x, half_x)],
                lines_y.at[to, pl.ds(h * half_x, half_x)],
                keep_x.at[h],
            ).start()

        load_x(1, 1).start()
        tables[0].wait()
        load_x(0, 0).wait()
        for n in range(0, part_z, 256):
            held[0, :, n : n + 256] = product(0, n)
        pl.semaphore_wait(barrier, n_left + n_right - 2)
        send_half(0, 0, 0)

        @pl.loop(1, part_y)
        def _(y):
            slot = y & 1

            @pl.when(y + 1 < part_y)
            def _():
                load_x(y + 1, 1 - slot).start()

            load_x(y, slot).wait()
            for n in range(0, part_z, 256):
                held[y, :, n : n + 256] = product(slot, n)
            send_half(y, 0, 0)

        @pl.loop(0, part_y - last_y)
        def _(y):
            send_half(y, 1, 1)

        @pl.loop(part_y - last_y, part_y)
        def _(y):
            send_half(y, 1, 2)

        def left_x(sem, planes):
            gone = lines_y.at[pl.ds(0, planes * (n_left - 1)), pl.ds(0, half_x)]
            pltpu.make_async_copy(gone, gone, send_x.at[sem]).wait()

        tables[1].wait()
        tables[2].wait()

        @pl.loop(0, size_z // inner)
        def _(outer):
            cos = turn[0, pl.ds(outer, 1), :]
            sin = turn[1, pl.ds(outer, 1), :]
            for c in range(0, size_z, LANES):
                value = cas[0, :, c : c + LANES] * cos + cas[1, :, c : c + LANES] * sin
                high, low = halves(value)
                big_high[pl.ds(outer * inner, inner), c : c + LANES] = high
                big_low[pl.ds(outer * inner, inner), c : c + LANES] = low

        rows = pl.multiple_of(right * rows_y, rows_y)
        column[...] = jnp.broadcast_to(sym_y[:, pl.ds(rows, rows_y)], (rows_y, rows_y)).T

        def arrived_x(h):
            part = pl.ds(h * half_x, half_x)
            own = lines_y.at[pl.ds(0, part_y), part]
            pltpu.make_async_copy(own, own, keep_x.at[h]).wait()
            others = lines_y.at[pl.ds(0, size_y - part_y), part]
            pltpu.make_async_copy(others, others, recv_x.at[h]).wait()

        def load_y(k, slot):
            return pltpu.make_async_copy(lines_y.at[:, k, :], taken.at[slot], load_sem.at[slot])

        columns = pl.ds(pl.multiple_of(right * part_z, part_z), part_z)

        def send_plane(k):
            for flip, sem in ((2, far_y.at[0, k]), (3, far_y.at[1, k]), (1, near_y.at[k])):
                peer = right ^ flip
                pltpu.make_async_remote_copy(
                    src_ref=result.at[k, :, pl.ds(pl.multiple_of(peer * part_z, part_z), part_z)],
                    dst_ref=lines_z.at[k, :, columns],
                    send_sem=send_y.at[k],
                    recv_sem=sem,
                    device_id={"right": peer},
                    device_id_type=MESH,
                ).start()
            pltpu.make_async_copy(result.at[k, :, columns], lines_z.at[k, :, columns], keep_y.at[k]).start()

        def transform_y(first, last, send):
            load_y(first, first & 1).start()

            @pl.loop(first, last)
            def _(k):
                slot = k & 1

                @pl.when(k + 1 < last)
                def _():
                    load_y(k + 1, 1 - slot).start()

                load_y(k, slot).wait()
                for n in range(0, part_z, 256):
                    value = product(slot, n)
                    for r in range(n_right):
                        result[k, :, r * part_z + n : r * part_z + n + 256] = value[r * rows_y : (r + 1) * rows_y]
                if send:
                    send_plane(k)

        arrived_x(0)
        transform_y(0, half_x, False)

        left_x(0, part_y)
        left_x(1, part_y - last_y)

        @pl.loop(0, half_x)
        def _(k):
            send_plane(k)

        arrived_x(1)
        transform_y(half_x, part_x, True)

        here = (right >> 1) * half_z
        pieces = (
            (here, half_z, line_in.at[0], stacked.at[0]),
            ((right ^ 2) * part_z, part_z, line_in.at[1, :, pl.ds(0, part_z)], stacked.at[1, :, pl.ds(0, part_z)]),
            ((right ^ 3) * part_z, part_z, line_in.at[1, :, pl.ds(part_z, part_z)], stacked.at[1, :, pl.ds(part_z, part_z)]),
        )

        def line(k, piece):
            start, depth, into, _ = pieces[piece]
            part = pl.ds(pl.multiple_of(start, part_z), depth)
            return pltpu.make_async_copy(lines_z.at[k, :, part], into, line_sem.at[piece])

        def stack(piece):
            high, low = halves(pieces[piece][2][...])
            pieces[piece][3][:rows_y] = high
            pieces[piece][3][rows_y:] = low

        def product_z(piece, cut):
            start, depth, _, both_halves = pieces[piece]
            part = pl.ds(pl.multiple_of(start, part_z), depth)
            both = dot(both_halves[...], big_high[part, cut])
            return both[:rows_y] + both[rows_y:] + dot(both_halves[:rows_y], big_low[part, cut])

        @pl.loop(0, part_x)
        def _(k):
            mine = lines_z.at[k, :, pl.ds(0, part_z)]
            pltpu.make_async_copy(mine, mine, keep_y.at[k]).wait()
            pltpu.make_async_copy(mine, mine, near_y.at[k]).wait()
            line(k, 0).start()
            line(k, 0).wait()
            stack(0)

            @pl.loop(0, size_z, step=512)
            def _(n):
                cut = pl.ds(pl.multiple_of(n, 512), 512)
                partial[:, cut] = product_z(0, cut)

            pltpu.make_async_copy(mine, mine, far_y.at[0, k]).wait()
            line(k, 1).start()
            line(k, 1).wait()
            stack(1)

            @pl.loop(0, size_z, step=512)
            def _(n):
                cut = pl.ds(pl.multiple_of(n, 512), 512)
                partial[:, cut] += product_z(1, cut)

            pltpu.make_async_copy(mine, mine, far_y.at[1, k]).wait()
            line(k, 2).start()
            sent = lines_z.at[k, :, pl.ds(0, size_z - part_z)]
            pltpu.make_async_copy(sent, sent, send_y.at[k]).wait()
            line(k, 2).wait()
            stack(2)
            sym_xy = sym_x[left * part_x + k] + column[...]

            @pl.loop(0, size_z, step=512)
            def _(n):
                cut = pl.ds(pl.multiple_of(n, 512), 512)
                total = partial[:, cut] + product_z(2, cut)
                for c in range(0, 512, LANES):
                    some = pl.ds(pl.multiple_of(n + c, LANES), LANES)
                    result[k, :, some] = total[:, c : c + LANES] * lax.rsqrt(sym_xy + sym_z[:, some])

        left_x(2, last_y)

    far = pl.BlockSpec(memory_space=pltpu.HBM)
    inside = pl.BlockSpec(memory_space=pltpu.VMEM)
    dma = pltpu.SemaphoreType.DMA
    return pl.pallas_call(
        kernel,
        out_shape=[
            jax.ShapeDtypeStruct((size_y, part_x, part_z), F32),
            jax.ShapeDtypeStruct((part_x, rows_y, size_z), F32),
            pltpu.VMEM((part_x, rows_y, size_z), F32),
        ],
        in_specs=[far] * 4 + [pl.BlockSpec(memory_space=pltpu.SMEM), inside, inside],
        out_specs=[far, far, inside],
        scratch_shapes=[
            pltpu.VMEM((part_y, size_x, part_z), F32),
            pltpu.VMEM((size_z, size_z), BF16),
            pltpu.VMEM((size_z, size_z), BF16),
            pltpu.VMEM((2, size_x, part_z), F32),
            pltpu.VMEM((2, rows_y, half_z), F32),
            pltpu.VMEM((2, 2 * rows_y, half_z), BF16),
            pltpu.VMEM((rows_y, size_z), F32),
            pltpu.VMEM((2, size_x, size_x), BF16),
            pltpu.VMEM((2, inner, size_z), F32),
            pltpu.VMEM((2, size_z // inner, LANES), F32),
            pltpu.VMEM((rows_y, rows_y), F32),
            dma((2,)), dma((3,)),
            dma((3,)), dma((2,)), dma((2,)),
            dma((part_x,)), dma((part_x,)), dma((2, part_x)), dma((part_x,)),
            dma((3,)),
        ],
        compiler_params=pltpu.CompilerParams(
            collective_id=0, has_side_effects=True, vmem_limit_bytes=46 * 1024 * 1024
        ),
        name="hartley",
    )


def solution(mesh):
    n_left, n_right = mesh.shape["left"], mesh.shape["right"]

    def per_device(density, symbol_x, symbol_y, symbol_z):
        size_x, size_y, size_z = density.shape[0], density.shape[1] * n_left, density.shape[2] * n_right
        small = jnp.asarray(small_table(size_x))
        cas, turn = (jnp.asarray(t) for t in factor_tables(size_z, 64))
        kernel = make_kernel(n_left, n_right, size_x, size_y, size_z)
        return kernel(density, small, cas, turn, symbol_x, symbol_y[None, :], symbol_z[None, :])[2]

    return jax.shard_map(
        per_device,
        mesh=mesh,
        in_specs=(P(None, "left", "right"), P(), P(), P()),
        out_specs=P("left", "right", None),
        check_vma=False,
    )
```

```python
import jax
import jax.numpy as jnp
import numpy as np
from jax import lax
from jax.experimental import pallas as pl
from jax.experimental.pallas import tpu as pltpu
from jax.sharding import PartitionSpec as P

MESH = pl.DeviceIdType.MESH
F32 = jnp.float32
BF16 = jnp.bfloat16
LANES = 128


def halves(value):
    high = value.astype(BF16)
    return high, (value - high.astype(F32)).astype(BF16)


def small_table(count):
    rank = np.arange(count)
    angle = 2.0 * np.pi / count * (rank[:, None] * rank[None, :] % count)
    table = ((np.cos(angle) + np.sin(angle)) * count ** (-0.5)).astype(np.float32)
    high = table.astype(BF16)
    low = (table - high.astype(np.float32)).astype(BF16)
    return np.stack([high, low])


def factor_tables(count, inner):
    rest, col = np.arange(inner), np.arange(count)
    angle = 2.0 * np.pi / count * (rest[:, None] * col[None, :] % count)
    scale = count ** (-0.5)
    plus = (np.cos(angle) + np.sin(angle)) * scale
    minus = (np.cos(angle) - np.sin(angle)) * scale
    outer = np.arange(count // inner)
    angle = 2.0 * np.pi / count * (outer[:, None] * inner * np.arange(LANES)[None, :] % count)
    return np.stack([plus, minus]).astype(np.float32), np.stack([np.cos(angle), np.sin(angle)]).astype(np.float32)


def dot(a, b):
    return jnp.dot(a, b, preferred_element_type=F32)


def make_kernel(n_left, n_right, size_x, size_y, size_z):
    part_x, part_y, rows_y, part_z = size_x // n_left, size_y // n_left, size_y // n_right, size_z // n_right
    half_x, half_z = part_x // 2, size_z // 2
    last_y = max(1, part_y // 2)
    inner = 64

    def partner(me, step):
        x = step & 3
        k = step >> 2
        z = (k ^ x) & 3
        y = ((k >> 2) ^ (x >> 1)) & 1
        return me ^ ((z << 3) | (y << 2) | x)

    def kernel(
        field, small_far, cas_far, turn_far, sym_x, sym_y, sym_z,
        lines_y, lines_z, result,
        held, big_high, big_low, taken, line_in, stacked, partial, small, cas, turn, column,
        load_sem, table_sem, send_x, recv_x, keep_x, send_y, near_y, far_y, keep_y, line_sem,
    ):
        left = lax.axis_index("left")
        right = lax.axis_index("right")

        def load_x(y, slot):
            return pltpu.make_async_copy(field.at[:, y, :], taken.at[slot], load_sem.at[slot])

        tables = [
            pltpu.make_async_copy(far, near, table_sem.at[i])
            for i, (far, near) in enumerate(((small_far, small), (cas_far, cas), (turn_far, turn)))
        ]
        load_x(0, 0).start()
        for copy in tables:
            copy.start()

        barrier = pltpu.get_barrier_semaphore()

        @pl.loop(1, n_left)
        def _(step):
            pl.semaphore_signal(barrier, inc=1, device_id={"left": partner(left, step)}, device_id_type=MESH)

        @pl.loop(1, n_right)
        def _(step):
            pl.semaphore_signal(barrier, inc=1, device_id={"right": right ^ step}, device_id_type=MESH)

        def product(slot, n):
            high, low = halves(taken[slot, :, n : n + 256])
            return dot(small[0], high) + dot(small[0], low) + dot(small[1], high)

        def send_half(y, h, sem):
            to = left * part_y + y

            @pl.loop(1, n_left)
            def _(step):
                peer = partner(left, step)
                pltpu.make_async_remote_copy(
                    src_ref=held.at[y, pl.ds(peer * part_x + h * half_x, half_x)],
                    dst_ref=lines_y.at[to, pl.ds(h * half_x, half_x)],
                    send_sem=send_x.at[sem],
                    recv_sem=recv_x.at[h],
                    device_id={"left": peer},
                    device_id_type=MESH,
                ).start()

            pltpu.make_async_copy(
                held.at[y, pl.ds(left * part_x + h * half_x, half_x)],
                lines_y.at[to, pl.ds(h * half_x, half_x)],
                keep_x.at[h],
            ).start()

        load_x(1, 1).start()
        tables[0].wait()
        load_x(0, 0).wait()
        for n in range(0, part_z, 256):
            held[0, :, n : n + 256] = product(0, n)
        pl.semaphore_wait(barrier, n_left + n_right - 2)
        send_half(0, 0, 0)

        @pl.loop(1, part_y)
        def _(y):
            slot = y & 1

            @pl.when(y + 1 < part_y)
            def _():
                load_x(y + 1, 1 - slot).start()

            load_x(y, slot).wait()
            for n in range(0, part_z, 256):
                held[y, :, n : n + 256] = product(slot, n)
            send_half(y, 0, 0)

        @pl.loop(0, part_y - last_y)
        def _(y):
            send_half(y, 1, 1)

        @pl.loop(part_y - last_y, part_y)
        def _(y):
            send_half(y, 1, 2)

        def left_x(sem, planes):
            gone = lines_y.at[pl.ds(0, planes * (n_left - 1)), pl.ds(0, half_x)]
            pltpu.make_async_copy(gone, gone, send_x.at[sem]).wait()

        tables[1].wait()
        tables[2].wait()

        @pl.loop(0, size_z // inner)
        def _(outer):
            cos = turn[0, pl.ds(outer, 1), :]
            sin = turn[1, pl.ds(outer, 1), :]
            for c in range(0, size_z, LANES):
                value = cas[0, :, c : c + LANES] * cos + cas[1, :, c : c + LANES] * sin
                high, low = halves(value)
                big_high[pl.ds(outer * inner, inner), c : c + LANES] = high
                big_low[pl.ds(outer * inner, inner), c : c + LANES] = low

        rows = pl.multiple_of(right * rows_y, rows_y)
        column[...] = jnp.broadcast_to(sym_y[:, pl.ds(rows, rows_y)], (rows_y, rows_y)).T

        def arrived_x(h):
            part = pl.ds(h * half_x, half_x)
            own = lines_y.at[pl.ds(0, part_y), part]
            pltpu.make_async_copy(own, own, keep_x.at[h]).wait()
            others = lines_y.at[pl.ds(0, size_y - part_y), part]
            pltpu.make_async_copy(others, others, recv_x.at[h]).wait()

        def load_y(k, slot):
            return pltpu.make_async_copy(lines_y.at[:, k, :], taken.at[slot], load_sem.at[slot])

        columns = pl.ds(pl.multiple_of(right * part_z, part_z), part_z)

        def send_plane(k):
            for flip, sem in ((2, far_y.at[0, k]), (3, far_y.at[1, k]), (1, near_y.at[k])):
                peer = right ^ flip
                pltpu.make_async_remote_copy(
                    src_ref=result.at[k, :, pl.ds(pl.multiple_of(peer * part_z, part_z), part_z)],
                    dst_ref=lines_z.at[k, :, columns],
                    send_sem=send_y.at[k],
                    recv_sem=sem,
                    device_id={"right": peer},
                    device_id_type=MESH,
                ).start()
            pltpu.make_async_copy(result.at[k, :, columns], lines_z.at[k, :, columns], keep_y.at[k]).start()

        def transform_y(first, last, send):
            load_y(first, first & 1).start()

            @pl.loop(first, last)
            def _(k):
                slot = k & 1

                @pl.when(k + 1 < last)
                def _():
                    load_y(k + 1, 1 - slot).start()

                load_y(k, slot).wait()
                for n in range(0, part_z, 256):
                    value = product(slot, n)
                    for r in range(n_right):
                        result[k, :, r * part_z + n : r * part_z + n + 256] = value[r * rows_y : (r + 1) * rows_y]
                if send:
                    send_plane(k)

        arrived_x(0)
        transform_y(0, half_x, False)

        left_x(0, part_y)
        left_x(1, part_y - last_y)

        @pl.loop(0, half_x)
        def _(k):
            send_plane(k)

        arrived_x(1)
        transform_y(half_x, part_x, True)

        here = (right >> 1) * half_z
        pieces = (
            (here, half_z, line_in.at[0], stacked.at[0]),
            ((right ^ 2) * part_z, part_z, line_in.at[1, :, pl.ds(0, part_z)], stacked.at[1, :, pl.ds(0, part_z)]),
            ((right ^ 3) * part_z, part_z, line_in.at[1, :, pl.ds(part_z, part_z)], stacked.at[1, :, pl.ds(part_z, part_z)]),
        )

        def line(k, piece):
            start, depth, into, _ = pieces[piece]
            part = pl.ds(pl.multiple_of(start, part_z), depth)
            return pltpu.make_async_copy(lines_z.at[k, :, part], into, line_sem.at[piece])

        def stack(piece):
            high, low = halves(pieces[piece][2][...])
            pieces[piece][3][:rows_y] = high
            pieces[piece][3][rows_y:] = low

        def product_z(piece, cut):
            start, depth, _, both_halves = pieces[piece]
            part = pl.ds(pl.multiple_of(start, part_z), depth)
            both = dot(both_halves[...], big_high[part, cut])
            return both[:rows_y] + both[rows_y:] + dot(both_halves[:rows_y], big_low[part, cut])

        @pl.loop(0, part_x)
        def _(k):
            mine = lines_z.at[k, :, pl.ds(0, part_z)]
            pltpu.make_async_copy(mine, mine, keep_y.at[k]).wait()
            pltpu.make_async_copy(mine, mine, near_y.at[k]).wait()
            line(k, 0).start()
            line(k, 0).wait()
            stack(0)

            @pl.loop(0, size_z, step=512)
            def _(n):
                cut = pl.ds(pl.multiple_of(n, 512), 512)
                partial[:, cut] = product_z(0, cut)

            pltpu.make_async_copy(mine, mine, far_y.at[0, k]).wait()
            line(k, 1).start()
            line(k, 1).wait()
            stack(1)

            @pl.loop(0, size_z, step=512)
            def _(n):
                cut = pl.ds(pl.multiple_of(n, 512), 512)
                partial[:, cut] += product_z(1, cut)

            pltpu.make_async_copy(mine, mine, far_y.at[1, k]).wait()
            line(k, 2).start()
            sent = lines_z.at[k, :, pl.ds(0, size_z - part_z)]
            pltpu.make_async_copy(sent, sent, send_y.at[k]).wait()
            line(k, 2).wait()
            stack(2)
            sym_xy = sym_x[left * part_x + k] + column[...]

            @pl.loop(0, size_z, step=512)
            def _(n):
                cut = pl.ds(pl.multiple_of(n, 512), 512)
                total = partial[:, cut] + product_z(2, cut)
                for c in range(0, 512, LANES):
                    some = pl.ds(pl.multiple_of(n + c, LANES), LANES)
                    result[k, :, some] = total[:, c : c + LANES] * lax.rsqrt(sym_xy + sym_z[:, some])

        left_x(2, last_y)

    far = pl.BlockSpec(memory_space=pltpu.HBM)
    inside = pl.BlockSpec(memory_space=pltpu.VMEM)
    dma = pltpu.SemaphoreType.DMA
    return pl.pallas_call(
        kernel,
        out_shape=[
            jax.ShapeDtypeStruct((size_y, part_x, part_z), F32),
            jax.ShapeDtypeStruct((part_x, rows_y, size_z), F32),
            pltpu.VMEM((part_x, rows_y, size_z), F32),
        ],
        in_specs=[far] * 4 + [pl.BlockSpec(memory_space=pltpu.SMEM), inside, inside],
        out_specs=[far, far, inside],
        scratch_shapes=[
            pltpu.VMEM((part_y, size_x, part_z), F32),
            pltpu.VMEM((size_z, size_z), BF16),
            pltpu.VMEM((size_z, size_z), BF16),
            pltpu.VMEM((2, size_x, part_z), F32),
            pltpu.VMEM((2, rows_y, half_z), F32),
            pltpu.VMEM((2, 2 * rows_y, half_z), BF16),
            pltpu.VMEM((rows_y, size_z), F32),
            pltpu.VMEM((2, size_x, size_x), BF16),
            pltpu.VMEM((2, inner, size_z), F32),
            pltpu.VMEM((2, size_z // inner, LANES), F32),
            pltpu.VMEM((rows_y, rows_y), F32),
            dma((2,)), dma((3,)),
            dma((3,)), dma((2,)), dma((2,)),
            dma((part_x,)), dma((part_x,)), dma((2, part_x)), dma((part_x,)),
            dma((3,)),
        ],
        compiler_params=pltpu.CompilerParams(
            collective_id=0, has_side_effects=True, vmem_limit_bytes=46 * 1024 * 1024
        ),
        name="hartley",
    )


def solution(mesh):
    n_left, n_right = mesh.shape["left"], mesh.shape["right"]

    def per_device(density, symbol_x, symbol_y, symbol_z):
        size_x, size_y, size_z = density.shape[0], density.shape[1] * n_left, density.shape[2] * n_right
        small = jnp.asarray(small_table(size_x))
        cas, turn = (jnp.asarray(t) for t in factor_tables(size_z, 64))
        kernel = make_kernel(n_left, n_right, size_x, size_y, size_z)
        return kernel(density, small, cas, turn, symbol_x, symbol_y[None, :], symbol_z[None, :])[2]

    return jax.shard_map(
        per_device,
        mesh=mesh,
        in_specs=(P(None, "left", "right"), P(), P(), P()),
        out_specs=P("left", "right", None),
        check_vma=False,
    )
```
